32 devices in a mesh: pb: 4 (over x, core), db: 8 (over z, y).
Axes of the slice: x: 2, y: 2, z: 4, core: 2. Of those that a mesh axis runs over, the one named last changes fastest.
Arguments:
- queries: bfloat16 [128, 1024], P(('pb', 'db')), may hold values from -6 to 6
- residual: bfloat16 [8192, 1024], P('db'), may hold values from -3 to 3
- codes: int32 [8192, 64], P('db'), may hold values from 0 to 255
- codebook: float32 [64, 256, 16], replicated, may hold values from -6 to 6
- ranks: int32 [128], P(('pb', 'db')), may hold values from 0 to 63
Outputs:
- hits: float32 [3, 128], P(None, ('pb', 'db'))
- totals: float32 [3], replicated
The draws below stay inside these ranges and needn't reach their ends.
All inputs are finite; a program needn't handle non-finite values.
Results may differ from the reference program's by a relative error of at most 0.00035.
Values may be sent and summed in bfloat16 or wider, within the bound.
No kernel may reach another device: no remote copies, remote signals or barrier semaphores. Data moves between devices by JAX's collectives and lax.ppermute only.
A program may use at most 128 MiB of HBM per device.

```python
import math
import jax
import jax.numpy as jnp
from jax import lax

SUBSPACES = 64
CENTROIDS = 256
SUBDIM = 16
D = 1024
LEVELS = 64
QUERIES = 128
DATABASE = 8192


def draw_ranks(key, part):
    base = jax.random.randint(jax.random.fold_in(key, 7), (QUERIES,), 0, LEVELS // 4)
    rising = jnp.arange(QUERIES, dtype=jnp.int32) * (3 * LEVELS // 4) // QUERIES
    return (base + rising).astype(jnp.int32)


def place_ends(entries, own_key, low, top_value):
    index_at = [jax.random.randint(jax.random.fold_in(own_key, axis), (), 0, length) for axis, length in enumerate(entries.shape)]
    longest = entries.shape.index(max(entries.shape))
    neighbour = index_at[:longest] + [(index_at[longest] + 1) % entries.shape[longest]] + index_at[longest + 1:]
    return entries.at[tuple(index_at)].set(low).at[tuple(neighbour)].set(top_value)


def steps_of(own_key, shape, shards, low, largest):
    factor_of, own = 1.0, jax.random.fold_in(own_key, 6)
    for axis_at, shards_of in shards:
        steps = jnp.exp(jax.random.uniform(jax.random.fold_in(own, axis_at), (shards_of,), jnp.float32, low / len(shards), largest / len(shards)))
        factor_of = factor_of * jnp.repeat(steps, shape[axis_at] // shards_of).reshape([-1 if axis == axis_at else 1 for axis in range(len(shape))])
    return factor_of


def noise(key, shape, scale, reach, shards=(), kind=jnp.bfloat16):
    drawn = scale * jax.random.normal(key, shape, jnp.float32)
    if shards:
        drawn = drawn * steps_of(key, shape, shards, -0.22, 0.18)
    return jnp.clip(drawn, -reach, reach).astype(kind)


def setup_inputs(seed: int = 0) -> dict:
    seeds = jax.random.split(jax.random.key(seed), 6)
    queries = noise(seeds[0], (QUERIES, D), 1.0, 6.0, ((0, 32),))
    residual = noise(seeds[1], (DATABASE, D), 0.5, 3.0, ((0, 8),))
    codes = place_ends(jax.random.randint(seeds[2], (DATABASE, SUBSPACES), 0, CENTROIDS), jax.random.fold_in(seeds[2], 1), 0, CENTROIDS - 1).astype(jnp.int32)
    codebook = noise(seeds[3], (SUBSPACES, CENTROIDS, SUBDIM), 1.0, 6.0, (), jnp.float32)
    ranks = draw_ranks(jax.random.fold_in(seeds[5], 71), 0)
    return {"queries": queries, "residual": residual, "codes": codes, "codebook": codebook, "ranks": ranks}


def pq_lookup(queries, codebook):
    count = queries.shape[0]
    subspaces, centroids, subdim = codebook.shape
    parts = queries.astype(jnp.float32).reshape(count, subspaces, subdim)
    query_parts = jnp.sum(parts * parts, axis=-1)
    centre_norms = jnp.sum(codebook * codebook, axis=-1)
    cross = jnp.einsum("qmj,mcj->qmc", parts, codebook, precision=lax.Precision.HIGHEST)
    lookup = (query_parts[:, :, None] + centre_norms[None] - 2.0 * cross) / (subspaces * subdim)
    return lookup.astype(jnp.bfloat16)


def reference(queries, residual, codes, codebook, ranks):
    subspace_ids = jnp.arange(SUBSPACES, dtype=jnp.int32)[None, :]
    recon = codebook[subspace_ids, codes].reshape(DATABASE, D)
    vectors = (recon + residual.astype(jnp.float32)).astype(jnp.bfloat16)
    vector_norms = jnp.sum(vectors.astype(jnp.float32) ** 2, axis=1)
    bounds = 1.9 + 0.6 * ranks.astype(jnp.float32) / (LEVELS - 1)
    query_size = math.gcd(QUERIES, 128)
    base_size = math.gcd(DATABASE, 1024)
    vector_blocks = vectors.reshape(DATABASE // base_size, base_size, D)
    norm_blocks = vector_norms.reshape(DATABASE // base_size, base_size)
    code_blocks = codes.reshape(DATABASE // base_size, base_size, SUBSPACES)

    def one_block(item):
        query_block, bound_block = item
        lookup = pq_lookup(query_block, codebook)
        query_norms = jnp.sum(query_block.astype(jnp.float32) ** 2, axis=1)

        def absorb(carry, piece):
            vector_piece, norm_piece, code_piece = piece
            picked = lookup[:, subspace_ids, code_piece].astype(jnp.float32)
            coarse = jnp.sum(picked, axis=-1)
            cross = jnp.dot(query_block, vector_piece.T, preferred_element_type=jnp.float32)
            exact = (query_norms[:, None] + norm_piece[None, :] - 2.0 * cross) / D
            exact_hit = jax.nn.sigmoid((bound_block[:, None] - exact) / 0.02)
            coarse_hit = jax.nn.sigmoid((bound_block[:, None] - coarse) / 0.02)
            part_sums = jnp.stack([jnp.sum(exact_hit, 1), jnp.sum(coarse_hit, 1), jnp.sum(exact_hit * coarse_hit, 1)])
            return carry + part_sums, None

        start = jnp.zeros((3, query_block.shape[0]), jnp.float32)
        result, _ = lax.scan(absorb, start, (vector_blocks, norm_blocks, code_blocks))
        return result

    sums = lax.map(one_block, (queries.reshape(QUERIES // query_size, query_size, D), bounds.reshape(QUERIES // query_size, query_size)))
    hits = jnp.transpose(sums, (1, 0, 2)).reshape(3, QUERIES) / DATABASE
    totals = jnp.sum(hits, axis=1) / QUERIES
    return hits, totals
```

```python
import functools

import jax
import jax.numpy as jnp
from jax import lax
from jax.experimental import pallas as pl
from jax.experimental.pallas import tpu as pltpu
from jax.sharding import PartitionSpec as P

LEVELS = 64
LANES = 128


def build_kernel(codes_ref, codebook_ref, residual_ref, recon_ref, vectors_ref, norms_ref):
    subspaces, subdim, centroids = codebook_ref.shape
    rows = codes_ref.shape[1]

    @pl.when(pl.program_id(0) == 0)
    def _():
        norms_ref[...] = jnp.zeros_like(norms_ref)

    def one_tile(tile, _):
        at = pl.ds(pl.multiple_of(tile * LANES, LANES), LANES)
        residual = residual_ref[at, :].astype(jnp.float32).T
        recon_norm = jnp.zeros((subdim, LANES), jnp.float32)
        vector_norm = jnp.zeros((subdim, LANES), jnp.float32)
        for m in range(subspaces):
            code = jnp.broadcast_to(codes_ref[m : m + 1, at], (subdim, LANES))
            lane = code % LANES
            recon = jnp.zeros((subdim, LANES), jnp.float32)
            for part in range(centroids // LANES):
                table = codebook_ref[m, :, part * LANES : (part + 1) * LANES]
                picked = jnp.take_along_axis(table, lane, axis=1, mode="promise_in_bounds")
                recon = jnp.where(code // LANES == part, picked, recon)
            features = slice(m * subdim, (m + 1) * subdim)
            vector = (recon + residual[features]).astype(jnp.bfloat16)
            wide = vector.astype(jnp.float32)
            recon_norm += recon * recon
            vector_norm += wide * wide
            recon_ref[features, at] = recon.astype(jnp.bfloat16)
            vectors_ref[features, at] = vector
        norms_ref[0:1, at] += jnp.sum(vector_norm, axis=0, keepdims=True)
        norms_ref[1:2, at] += jnp.sum(recon_norm, axis=0, keepdims=True)
        return 0

    lax.fori_loop(0, rows // LANES, one_tile, 0)


def build(codes, codebook, residual):
    subspaces, subdim, centroids = codebook.shape
    rows, width = residual.shape
    group = LANES // subdim
    return pl.pallas_call(
        build_kernel,
        grid=(subspaces // group,),
        in_specs=[
            pl.BlockSpec((group, rows), lambda g: (g, 0)),
            pl.BlockSpec((group, subdim, centroids), lambda g: (g, 0, 0)),
            pl.BlockSpec((rows, LANES), lambda g: (0, g)),
        ],
        out_specs=[
            pl.BlockSpec((LANES, rows), lambda g: (g, 0)),
            pl.BlockSpec((LANES, rows), lambda g: (g, 0)),
            pl.BlockSpec((8, rows), lambda g: (0, 0)),
        ],
        out_shape=[
            jax.ShapeDtypeStruct((width, rows), jnp.bfloat16),
            jax.ShapeDtypeStruct((width, rows), jnp.bfloat16),
            jax.ShapeDtypeStruct((8, rows), jnp.float32),
        ],
        compiler_params=pltpu.CompilerParams(
            dimension_semantics=("arbitrary",), vmem_limit_bytes=8 * 2**20
        ),
        cost_estimate=pl.CostEstimate(
            flops=32 * rows * width, bytes_accessed=8 * rows * width, transcendentals=0
        ),
        name="build",
    )(codes, codebook, residual)


def count_kernel(visiting_ref, recon_ref, vectors_ref, norms_ref, out_ref, gathered):
    senders, count, packed = visiting_ref.shape
    width = recon_ref.shape[0]
    for s in range(senders):
        gathered[s * count : (s + 1) * count, :] = visiting_ref[s].astype(jnp.float32)
    queries = gathered[:, :width]
    query_norms = jnp.sum(queries * queries, axis=1, keepdims=True)
    bounds = 1.9 + 0.6 * gathered[:, width : width + 1] / (LEVELS - 1)
    queries = queries.astype(jnp.bfloat16)

    def hit(values_ref, norms):
        cross = jnp.dot(queries, values_ref[...], preferred_element_type=jnp.float32)
        distance = (query_norms + norms - 2.0 * cross) / width
        return jax.nn.sigmoid((bounds - distance) / 0.02)

    exact = hit(vectors_ref, norms_ref[0:1, :])
    coarse = hit(recon_ref, norms_ref[1:2, :])
    lane = lax.broadcasted_iota(jnp.int32, (senders * count, LANES), 1)
    query = lax.broadcasted_iota(jnp.int32, (senders * count, LANES), 0)
    blocks = jnp.zeros((senders * count, LANES), jnp.float32)
    sums = jnp.zeros((1, LANES), jnp.float32)
    for k, values in enumerate((exact, coarse, exact * coarse)):
        total = jnp.sum(values, axis=1, keepdims=True)
        blocks = jnp.where(lane == k * count + query % count, total, blocks)
        sums = jnp.where(lane[:1] == 3 * count + k, jnp.sum(total, axis=0, keepdims=True), sums)
    for s in range(senders):
        row = jnp.sum(blocks[s * count : (s + 1) * count], axis=0, keepdims=True) + sums
        for p in range(out_ref.shape[0]):
            out_ref[p, s] = row


def per_device(queries, residual, codes, codebook, ranks):
    count, width = queries.shape
    rows = residual.shape[0]
    shards, copies = lax.axis_size("db"), lax.axis_size("pb")
    devices = shards * copies
    assert 3 * count + 3 <= LANES

    own_ranks = jnp.broadcast_to(ranks.astype(jnp.bfloat16)[:, None], (count, LANES))
    packed = jnp.concatenate([queries, own_ranks], axis=1)
    visiting = lax.all_to_all(
        jnp.broadcast_to(packed[None], (shards, *packed.shape)), "db", 0, 0
    )
    recon, vectors, norms = build(codes.T, jnp.transpose(codebook, (0, 2, 1)), residual)
    partial_sums = pl.pallas_call(
        count_kernel,
        out_shape=jax.ShapeDtypeStruct((copies, shards, 1, LANES), jnp.float32),
        scratch_shapes=[pltpu.VMEM((shards * count, width + LANES), jnp.float32)],
        compiler_params=pltpu.CompilerParams(vmem_limit_bytes=16 * 2**20),
        cost_estimate=pl.CostEstimate(
            flops=4 * shards * count * rows * width,
            bytes_accessed=4 * rows * width,
            transcendentals=0,
        ),
        name="count",
    )(visiting, recon, vectors, norms)
    arrived = lax.all_to_all(
        partial_sums.reshape(devices, 1, LANES), ("pb", "db"), 0, 0
    ).reshape(copies, shards, LANES)
    own = jnp.arange(copies)[:, None, None] == lax.axis_index("pb")
    hits = jnp.sum(jnp.where(own, arrived, 0.0), axis=(0, 1))[: 3 * count].reshape(3, count)
    totals = jnp.sum(arrived, axis=(0, 1))[3 * count : 3 * count + 3]
    database = rows * shards
    return hits / database, totals / (database * count * devices)


def solution(mesh):
    return jax.shard_map(
        per_device,
        mesh=mesh,
        in_specs=(P(("pb", "db"), None), P("db", None), P("db", None), P(), P(("pb", "db"))),
        out_specs=(P(None, ("pb", "db")), P()),
        check_vma=False,
    )
```

```python
import functools

import jax
import jax.numpy as jnp
from jax import lax
from jax.experimental import pallas as pl
from jax.experimental.pallas import tpu as pltpu
from jax.sharding import PartitionSpec as P

LEVELS = 64
LANES = 128


def in_hbm(array):
    return pltpu.with_memory_space_constraint(array, pltpu.HBM)


def pack_kernel(queries_hbm, ranks_hbm, out_ref, queries, ranks, sems):
    count, width = queries.shape
    copies = (
        pltpu.make_async_copy(queries_hbm, queries, sems.at[0]),
        pltpu.make_async_copy(ranks_hbm, ranks, sems.at[1]),
    )
    for copy in copies:
        copy.start()
    for copy in copies:
        copy.wait()
    for i in range(count):
        rank = jnp.full((1, LANES), ranks[i], jnp.int32).astype(jnp.float32)
        for s in range(out_ref.shape[0]):
            out_ref[s, i : i + 1, width:] = rank.astype(jnp.bfloat16)
    for s in range(out_ref.shape[0]):
        out_ref[s, :, :width] = queries[...]


def pack(queries, ranks, receivers):
    count, width = queries.shape
    return pl.pallas_call(
        pack_kernel,
        in_specs=[pl.BlockSpec(memory_space=pltpu.HBM)] * 2,
        out_shape=jax.ShapeDtypeStruct((receivers, count, width + LANES), jnp.bfloat16),
        scratch_shapes=[
            pltpu.VMEM(queries.shape, queries.dtype),
            pltpu.SMEM(ranks.shape, ranks.dtype),
            pltpu.SemaphoreType.DMA((2,)),
        ],
        compiler_params=pltpu.CompilerParams(vmem_limit_bytes=8 * 2**20),
        name="pack",
    )(in_hbm(queries), in_hbm(ranks))


def build_kernel(
    codes_hbm, codebook_hbm, residual_hbm, values_ref, norms_ref, codes, codebook, residual, sems
):
    subspaces, subdim, centroids = codebook.shape
    rows, width = residual.shape
    group = LANES // subdim
    groups = subspaces // group
    share = lax.rem(lax.axis_index("pb"), codes_hbm.shape[1] // rows)
    own = pl.ds(pl.multiple_of(share * rows, rows), rows)

    def copies(g):
        members = pl.ds(pl.multiple_of(g * group, group), group)
        features = pl.ds(pl.multiple_of(g * LANES, LANES), LANES)
        return (
            pltpu.make_async_copy(codes_hbm.at[members, own], codes.at[g], sems.at[0, g]),
            pltpu.make_async_copy(codebook_hbm.at[members], codebook.at[members], sems.at[1, g]),
            pltpu.make_async_copy(
                residual_hbm.at[own, features], residual.at[:, features], sems.at[2, g]
            ),
        )

    for g in range(groups):
        for copy in copies(g):
            copy.start()
    norms_ref[...] = jnp.zeros_like(norms_ref)
    row = lax.broadcasted_iota(jnp.int32, (LANES, LANES), 0)
    column = lax.broadcasted_iota(jnp.int32, (LANES, LANES), 1)
    identity = (row == column).astype(jnp.bfloat16)

    def one_group(g, _):
        for copy in copies(g):
            copy.wait()
        first = pl.multiple_of(g * LANES, LANES)
        for tile in range(rows // LANES):
            at = slice(tile * LANES, (tile + 1) * LANES)
            turned = lax.dot_general(
                identity,
                residual[at, pl.ds(first, LANES)],
                (((1,), (1,)), ((), ())),
                preferred_element_type=jnp.float32,
            )
            recon_norm = jnp.zeros((subdim, LANES), jnp.float32)
            vector_norm = jnp.zeros((subdim, LANES), jnp.float32)
            for m in range(group):
                code = jnp.broadcast_to(codes[g, m : m + 1, at], (subdim, LANES))
                lane = code & (LANES - 1)
                recon = None
                for part in range(centroids // LANES):
                    table = codebook[g * group + m, :, part * LANES : (part + 1) * LANES]
                    picked = jnp.take_along_axis(table, lane, axis=1, mode="promise_in_bounds")
                    recon = picked if part == 0 else jnp.where(code >= part * LANES, picked, recon)
                vector = (recon + turned[m * subdim : (m + 1) * subdim]).astype(jnp.bfloat16)
                wide = vector.astype(jnp.float32)
                recon_norm += recon * recon
                vector_norm += wide * wide
                features = pl.ds(first + m * subdim, subdim)
                values_ref[0, features, at] = vector
                values_ref[1, features, at] = recon.astype(jnp.bfloat16)
            norms_ref[0:8, at] += sum(vector_norm[i : i + 8] for i in range(0, subdim, 8))
            norms_ref[8:16, at] += sum(recon_norm[i : i + 8] for i in range(0, subdim, 8))
        return 0

    lax.fori_loop(0, groups, one_group, 0)


def build(codes, codebook, residual, fold):
    subspaces, subdim, centroids = codebook.shape
    rows, width = residual.shape[0] // fold, residual.shape[1]
    groups = subspaces * subdim // LANES
    assert LANES % subdim == 0 and subdim % 8 == 0 and centroids % LANES == 0 and rows % LANES == 0
    return pl.pallas_call(
        build_kernel,
        in_specs=[pl.BlockSpec(memory_space=pltpu.HBM)] * 3,
        out_specs=[pl.BlockSpec(memory_space=pltpu.VMEM)] * 2,
        out_shape=[
            jax.ShapeDtypeStruct((2, width, rows), jnp.bfloat16),
            jax.ShapeDtypeStruct((16, rows), jnp.float32),
        ],
        scratch_shapes=[
            pltpu.VMEM((groups, LANES // subdim, rows), codes.dtype),
            pltpu.VMEM(codebook.shape, codebook.dtype),
            pltpu.VMEM((rows, width), residual.dtype),
            pltpu.SemaphoreType.DMA((3, groups)),
        ],
        compiler_params=pltpu.CompilerParams(vmem_limit_bytes=16 * 2**20),
        cost_estimate=pl.CostEstimate(
            flops=32 * rows * width, bytes_accessed=8 * rows * width, transcendentals=0
        ),
        name="build",
    )(in_hbm(codes), in_hbm(codebook), in_hbm(residual))


def count_kernel(visiting_ref, values_ref, norms_ref, out_ref, gathered):
    senders, count, packed = visiting_ref.shape
    width = values_ref.shape[1]
    for s in range(senders):
        gathered[s * count : (s + 1) * count, :] = visiting_ref[s].astype(jnp.float32)
    queries = gathered[:, :width]
    query_norms = jnp.sum(queries * queries, axis=1, keepdims=True)
    bounds = 1.9 + 0.6 * gathered[:, width : width + 1] / (LEVELS - 1)
    queries = queries.astype(jnp.bfloat16)

    def hit(kind):
        norms = jnp.sum(norms_ref[kind * 8 : kind * 8 + 8], axis=0, keepdims=True)
        cross = jnp.dot(queries, values_ref[kind], preferred_element_type=jnp.float32)
        distance = (query_norms + norms - 2.0 * cross) / width
        return jax.nn.sigmoid((bounds - distance) / 0.02)

    exact = hit(0)
    coarse = hit(1)
    lane = lax.broadcasted_iota(jnp.int32, (senders * count, LANES), 1)
    query = lax.broadcasted_iota(jnp.int32, (senders * count, LANES), 0)
    blocks = jnp.zeros((senders * count, LANES), jnp.float32)
    sums = jnp.zeros((1, LANES), jnp.float32)
    for k, values in enumerate((exact, coarse, exact * coarse)):
        total = jnp.sum(values, axis=1, keepdims=True)
        blocks = jnp.where(lane == k * count + query % count, total, blocks)
        sums = jnp.where(lane[:1] == 3 * count + k, jnp.sum(total, axis=0, keepdims=True), sums)
    for s in range(senders):
        row = jnp.sum(blocks[s * count : (s + 1) * count], axis=0, keepdims=True) + sums
        for p in range(out_ref.shape[0]):
            out_ref[p, s] = row


def finish_kernel(fold, database, everyone, arrived_ref, hits_ref, totals_ref):
    copies, shards = arrived_ref.shape[:2]
    count = hits_ref.shape[1]
    mine = lax.axis_index("pb") // fold
    hits = jnp.zeros((1, LANES), jnp.float32)
    totals = jnp.zeros((1, LANES), jnp.float32)
    for p in range(copies):
        arrived = jnp.sum(arrived_ref[p], axis=0)
        hits += jnp.where(mine == p // fold, arrived, 0.0)
        totals += arrived
    hits = hits / database
    totals = totals / (database * everyone)
    for k in range(3):
        hits_ref[k : k + 1, :] = hits[:, k * count : (k + 1) * count]
    totals_ref[...] = totals[:, 3 * count : 3 * count + 3]


def per_device(queries, residual, codes, codebook, ranks):
    count, width = queries.shape
    shards, copies = lax.axis_size("db"), lax.axis_size("pb")
    devices = shards * copies
    fold = 2 if copies % 2 == 0 and residual.shape[0] % (2 * LANES) == 0 else 1
    rows = residual.shape[0] // fold
    senders = fold * shards
    assert 3 * count + 3 <= LANES

    groups = [list(range(first, first + senders)) for first in range(0, devices, senders)]
    visiting = lax.all_to_all(
        pack(queries, ranks, senders), ("pb", "db"), 0, 0, axis_index_groups=groups
    )
    values, norms = build(codes.T, jnp.transpose(codebook, (0, 2, 1)), residual, fold)
    partial_sums = pl.pallas_call(
        count_kernel,
        out_shape=jax.ShapeDtypeStruct((copies // fold, senders, 1, LANES), jnp.float32),
        scratch_shapes=[pltpu.VMEM((senders * count, width + LANES), jnp.float32)],
        compiler_params=pltpu.CompilerParams(vmem_limit_bytes=16 * 2**20),
        cost_estimate=pl.CostEstimate(
            flops=4 * senders * count * rows * width,
            bytes_accessed=4 * rows * width,
            transcendentals=0,
        ),
        name="count",
    )(visiting, values, norms)
    arrived = lax.all_to_all(partial_sums.reshape(devices, 1, LANES), ("pb", "db"), 0, 0)
    hits, totals = pl.pallas_call(
        functools.partial(finish_kernel, fold, rows * senders, count * devices),
        out_shape=[
            jax.ShapeDtypeStruct((3, count), jnp.float32),
            jax.ShapeDtypeStruct((1, 3), jnp.float32),
        ],
        compiler_params=pltpu.CompilerParams(vmem_limit_bytes=8 * 2**20),
        name="finish",
    )(arrived.reshape(copies, shards, 1, LANES))
    return hits, totals[0]


def solution(mesh):
    return jax.shard_map(
        per_device,
        mesh=mesh,
        in_specs=(P(("pb", "db"), None), P("db", None), P("db", None), P(), P(("pb", "db"))),
        out_specs=(P(None, ("pb", "db")), P()),
        check_vma=False,
    )
```

```python
import functools

import jax
import jax.numpy as jnp
from jax import lax
from jax.experimental import pallas as pl
from jax.experimental.pallas import tpu as pltpu
from jax.sharding import PartitionSpec as P

LEVELS = 64
LANES = 128


def in_hbm(array):
    return pltpu.with_memory_space_constraint(array, pltpu.HBM)


def pack_kernel(queries_hbm, ranks_hbm, out_ref, queries, ranks, sems):
    count, width = queries.shape
    copies = (
        pltpu.make_async_copy(queries_hbm, queries, sems.at[0]),
        pltpu.make_async_copy(ranks_hbm, ranks, sems.at[1]),
    )
    for copy in copies:
        copy.start()
    for copy in copies:
        copy.wait()
    for i in range(count):
        rank = jnp.full((1, LANES), ranks[i], jnp.int32).astype(jnp.float32)
        for s in range(out_ref.shape[0]):
            out_ref[s, i : i + 1, width:] = rank.astype(jnp.bfloat16)
    for s in range(out_ref.shape[0]):
        out_ref[s, :, :width] = queries[...]


def pack(queries, ranks, receivers):
    count, width = queries.shape
    return pl.pallas_call(
        pack_kernel,
        in_specs=[pl.BlockSpec(memory_space=pltpu.HBM)] * 2,
        out_shape=jax.ShapeDtypeStruct((receivers, count, width + LANES), jnp.bfloat16),
        scratch_shapes=[
            pltpu.VMEM(queries.shape, queries.dtype),
            pltpu.SMEM(ranks.shape, ranks.dtype),
            pltpu.SemaphoreType.DMA((2,)),
        ],
        compiler_params=pltpu.CompilerParams(vmem_limit_bytes=8 * 2**20),
        name="pack",
    )(in_hbm(queries), in_hbm(ranks))


def build_kernel(
    codes_hbm, codebook_hbm, residual_hbm, values_ref, norms_ref, codes, codebook, residual, sems
):
    subspaces, subdim, centroids = codebook.shape
    rows, width = residual.shape
    group = LANES // subdim
    groups = subspaces // group
    share = lax.rem(lax.axis_index("pb"), codes_hbm.shape[1] // rows)
    own = pl.ds(pl.multiple_of(share * rows, rows), rows)

    def copies(g):
        members = pl.ds(pl.multiple_of(g * group, group), group)
        features = pl.ds(pl.multiple_of(g * LANES, LANES), LANES)
        return (
            pltpu.make_async_copy(codes_hbm.at[members, own], codes.at[g], sems.at[0, g]),
            pltpu.make_async_copy(codebook_hbm.at[members], codebook.at[members], sems.at[1, g]),
            pltpu.make_async_copy(
                residual_hbm.at[own, features], residual.at[:, features], sems.at[2, g]
            ),
        )

    for g in range(groups):
        for copy in copies(g):
            copy.start()
    norms_ref[...] = jnp.zeros_like(norms_ref)
    row = lax.broadcasted_iota(jnp.int32, (LANES, LANES), 0)
    column = lax.broadcasted_iota(jnp.int32, (LANES, LANES), 1)
    identity = (row == column).astype(jnp.bfloat16)

    def one_group(g, _):
        for copy in copies(g):
            copy.wait()
        first = pl.multiple_of(g * LANES, LANES)
        for tile in range(rows // LANES):
            at = slice(tile * LANES, (tile + 1) * LANES)
            turned = lax.dot_general(
                identity,
                residual[at, pl.ds(first, LANES)],
                (((1,), (1,)), ((), ())),
                preferred_element_type=jnp.float32,
            )
            recon_norm = jnp.zeros((subdim, LANES), jnp.float32)
            vector_norm = jnp.zeros((subdim, LANES), jnp.float32)
            for m in range(group):
                code = jnp.broadcast_to(codes[g, m : m + 1, at], (subdim, LANES))
                lane = code & (LANES - 1)
                recon = None
                for part in range(centroids // LANES):
                    table = codebook[g * group + m, :, part * LANES : (part + 1) * LANES]
                    picked = jnp.take_along_axis(table, lane, axis=1, mode="promise_in_bounds")
                    recon = picked if part == 0 else jnp.where(code >= part * LANES, picked, recon)
                vector = (recon + turned[m * subdim : (m + 1) * subdim]).astype(jnp.bfloat16)
                wide = vector.astype(jnp.float32)
                recon_norm += recon * recon
                vector_norm += wide * wide
                features = pl.ds(first + m * subdim, subdim)
                values_ref[0, features, at] = vector
                values_ref[1, features, at] = recon.astype(jnp.bfloat16)
            norms_ref[0:8, at] += sum(vector_norm[i : i + 8] for i in range(0, subdim, 8))
            norms_ref[8:16, at] += sum(recon_norm[i : i + 8] for i in range(0, subdim, 8))
        return 0

    lax.fori_loop(0, groups, one_group, 0)


def build(codes, codebook, residual, fold):
    subspaces, subdim, centroids = codebook.shape
    rows, width = residual.shape[0] // fold, residual.shape[1]
    groups = subspaces * subdim // LANES
    assert LANES % subdim == 0 and subdim % 8 == 0 and centroids % LANES == 0 and rows % LANES == 0
    return pl.pallas_call(
        build_kernel,
        in_specs=[pl.BlockSpec(memory_space=pltpu.HBM)] * 3,
        out_specs=[pl.BlockSpec(memory_space=pltpu.VMEM)] * 2,
        out_shape=[
            jax.ShapeDtypeStruct((2, width, rows), jnp.bfloat16),
            jax.ShapeDtypeStruct((16, rows), jnp.float32),
        ],
        scratch_shapes=[
            pltpu.VMEM((groups, LANES // subdim, rows), codes.dtype),
            pltpu.VMEM(codebook.shape, codebook.dtype),
            pltpu.VMEM((rows, width), residual.dtype),
            pltpu.SemaphoreType.DMA((3, groups)),
        ],
        compiler_params=pltpu.CompilerParams(vmem_limit_bytes=16 * 2**20),
        cost_estimate=pl.CostEstimate(
            flops=32 * rows * width, bytes_accessed=8 * rows * width, transcendentals=0
        ),
        name="build",
    )(in_hbm(codes), in_hbm(codebook), in_hbm(residual))


def count_kernel(order, visiting_ref, values_ref, norms_ref, out_ref, gathered):
    senders, count, packed = visiting_ref.shape
    width = values_ref.shape[1]
    for s in range(senders):
        gathered[s * count : (s + 1) * count, :] = visiting_ref[s].astype(jnp.float32)
    queries = gathered[:, :width]
    query_norms = jnp.sum(queries * queries, axis=1, keepdims=True)
    bounds = 1.9 + 0.6 * gathered[:, width : width + 1] / (LEVELS - 1)
    queries = queries.astype(jnp.bfloat16)

    def hit(kind):
        norms = jnp.sum(norms_ref[kind * 8 : kind * 8 + 8], axis=0, keepdims=True)
        cross = jnp.dot(queries, values_ref[kind], preferred_element_type=jnp.float32)
        distance = (query_norms + norms - 2.0 * cross) / width
        return jax.nn.sigmoid((bounds - distance) / 0.02)

    exact = hit(0)
    coarse = hit(1)
    lane = lax.broadcasted_iota(jnp.int32, (senders * count, LANES), 1)
    query = lax.broadcasted_iota(jnp.int32, (senders * count, LANES), 0)
    blocks = jnp.zeros((senders * count, LANES), jnp.float32)
    sums = jnp.zeros((1, LANES), jnp.float32)
    for k, values in enumerate((exact, coarse, exact * coarse)):
        total = jnp.sum(values, axis=1, keepdims=True)
        blocks = jnp.where(lane == k * count + query % count, total, blocks)
        sums = jnp.where(lane[:1] == 3 * count + k, jnp.sum(total, axis=0, keepdims=True), sums)
    for s in range(senders):
        row = jnp.sum(blocks[s * count : (s + 1) * count], axis=0, keepdims=True) + sums
        for p in range(out_ref.shape[0]):
            out_ref[p, order[s]] = row


def finish_kernel(fold, database, everyone, arrived_ref, hits_ref, totals_ref):
    copies, shards = arrived_ref.shape[:2]
    count = hits_ref.shape[1]
    mine = lax.axis_index("pb") // fold
    hits = jnp.zeros((1, LANES), jnp.float32)
    totals = jnp.zeros((1, LANES), jnp.float32)
    for p in range(copies):
        arrived = jnp.sum(arrived_ref[p], axis=0)
        hits += jnp.where(mine == p // fold, arrived, 0.0)
        totals += arrived
    hits = hits / database
    totals = totals / (database * everyone)
    for k in range(3):
        hits_ref[k : k + 1, :] = hits[:, k * count : (k + 1) * count]
    totals_ref[...] = totals[:, 3 * count : 3 * count + 3]


def per_device(queries, residual, codes, codebook, ranks):
    count, width = queries.shape
    shards, copies = lax.axis_size("db"), lax.axis_size("pb")
    devices = shards * copies
    fold = 2 if copies % 2 == 0 and residual.shape[0] % (2 * LANES) == 0 else 1
    rows = residual.shape[0] // fold
    senders = fold * shards
    assert 3 * count + 3 <= LANES

    order = list(range(senders))
    order.insert(0, order.pop(senders - shards // 2))
    groups = [[first + at for at in order] for first in range(0, devices, senders)]
    visiting = lax.all_to_all(
        pack(queries, ranks, senders), ("pb", "db"), 0, 0, axis_index_groups=groups
    )
    values, norms = build(codes.T, jnp.transpose(codebook, (0, 2, 1)), residual, fold)
    partial_sums = pl.pallas_call(
        functools.partial(count_kernel, order),
        out_shape=jax.ShapeDtypeStruct((copies // fold, senders, 1, LANES), jnp.float32),
        scratch_shapes=[pltpu.VMEM((senders * count, width + LANES), jnp.float32)],
        compiler_params=pltpu.CompilerParams(vmem_limit_bytes=16 * 2**20),
        cost_estimate=pl.CostEstimate(
            flops=4 * senders * count * rows * width,
            bytes_accessed=4 * rows * width,
            transcendentals=0,
        ),
        name="count",
    )(visiting, values, norms)
    arrived = lax.all_to_all(partial_sums.reshape(devices, 1, LANES), ("pb", "db"), 0, 0)
    hits, totals = pl.pallas_call(
        functools.partial(finish_kernel, fold, rows * senders, count * devices),
        out_shape=[
            jax.ShapeDtypeStruct((3, count), jnp.float32),
            jax.ShapeDtypeStruct((1, 3), jnp.float32),
        ],
        compiler_params=pltpu.CompilerParams(vmem_limit_bytes=8 * 2**20),
        name="finish",
    )(arrived.reshape(copies, shards, 1, LANES))
    return hits, totals[0]


def solution(mesh):
    return jax.shard_map(
        per_device,
        mesh=mesh,
        in_specs=(P(("pb", "db"), None), P("db", None), P("db", None), P(), P(("pb", "db"))),
        out_specs=(P(None, ("pb", "db")), P()),
        check_vma=False,
    )
```

```python
import functools

import jax
import jax.numpy as jnp
from jax import lax
from jax.experimental import pallas as pl
from jax.experimental.pallas import tpu as pltpu
from jax.sharding import PartitionSpec as P

LEVELS = 64
LANES = 128


def in_hbm(array):
    return pltpu.with_memory_space_constraint(array, pltpu.HBM)


def pack_kernel(queries_hbm, ranks_hbm, out_ref, queries, ranks, sems):
    count, width = queries.shape
    copies = (
        pltpu.make_async_copy(ranks_hbm, ranks, sems.at[1]),
        pltpu.make_async_copy(queries_hbm, queries, sems.at[0]),
    )
    for copy in copies:
        copy.start()
    for copy in copies:
        copy.wait()
    for i in range(count):
        rank = jnp.full((1, LANES), ranks[i], jnp.int32).astype(jnp.float32)
        for s in range(out_ref.shape[0]):
            out_ref[s, i : i + 1, width:] = rank.astype(jnp.bfloat16)
    for s in range(out_ref.shape[0]):
        out_ref[s, :, :width] = queries[...]


def pack(queries, ranks, receivers):
    count, width = queries.shape
    return pl.pallas_call(
        pack_kernel,
        in_specs=[pl.BlockSpec(memory_space=pltpu.HBM)] * 2,
        out_shape=jax.ShapeDtypeStruct((receivers, count, width + LANES), jnp.bfloat16),
        scratch_shapes=[
            pltpu.VMEM(queries.shape, queries.dtype),
            pltpu.SMEM(ranks.shape, ranks.dtype),
            pltpu.SemaphoreType.DMA((2,)),
        ],
        compiler_params=pltpu.CompilerParams(vmem_limit_bytes=8 * 2**20),
        name="pack",
    )(in_hbm(queries), in_hbm(ranks))


def build_kernel(
    codes_hbm, codebook_hbm, residual_hbm, values_ref, norms_ref, codes, codebook, residual, sems
):
    subspaces, subdim, centroids = codebook.shape
    rows, width = residual.shape
    group = LANES // subdim
    groups = subspaces // group
    share = lax.rem(lax.axis_index("pb"), codes_hbm.shape[1] // rows)
    own = pl.ds(pl.multiple_of(share * rows, rows), rows)

    def copies(g):
        members = pl.ds(pl.multiple_of(g * group, group), group)
        features = pl.ds(pl.multiple_of(g * LANES, LANES), LANES)
        return (
            pltpu.make_async_copy(codes_hbm.at[members, own], codes.at[g], sems.at[0, g]),
            pltpu.make_async_copy(codebook_hbm.at[members], codebook.at[members], sems.at[1, g]),
            pltpu.make_async_copy(
                residual_hbm.at[own, features], residual.at[:, features], sems.at[2, g]
            ),
        )

    for g in range(groups):
        for copy in copies(g):
            copy.start()
    norms_ref[...] = jnp.zeros_like(norms_ref)
    row = lax.broadcasted_iota(jnp.int32, (LANES, LANES), 0)
    column = lax.broadcasted_iota(jnp.int32, (LANES, LANES), 1)
    identity = (row == column).astype(jnp.bfloat16)

    def one_group(g, _):
        for copy in copies(g):
            copy.wait()
        first = pl.multiple_of(g * LANES, LANES)
        for tile in range(rows // LANES):
            at = slice(tile * LANES, (tile + 1) * LANES)
            turned = lax.dot_general(
                identity,
                residual[at, pl.ds(first, LANES)],
                (((1,), (1,)), ((), ())),
                preferred_element_type=jnp.float32,
            )
            recon_norm = jnp.zeros((subdim, LANES), jnp.float32)
            vector_norm = jnp.zeros((subdim, LANES), jnp.float32)
            for m in range(group):
                code = jnp.broadcast_to(codes[g, m : m + 1, at], (subdim, LANES))
                lane = code & (LANES - 1)
                recon = None
                for part in range(centroids // LANES):
                    table = codebook[g * group + m, :, part * LANES : (part + 1) * LANES]
                    picked = jnp.take_along_axis(table, lane, axis=1, mode="promise_in_bounds")
                    recon = picked if part == 0 else jnp.where(code >= part * LANES, picked, recon)
                vector = (recon + turned[m * subdim : (m + 1) * subdim]).astype(jnp.bfloat16)
                rounded = recon.astype(jnp.bfloat16)
                recon_norm += rounded.astype(jnp.float32) ** 2
                vector_norm += vector.astype(jnp.float32) ** 2
                features = pl.ds(first + m * subdim, subdim)
                values_ref[0, features, at] = vector
                values_ref[1, features, at] = rounded
            norms_ref[0:8, at] += sum(vector_norm[i : i + 8] for i in range(0, subdim, 8))
            norms_ref[8:16, at] += sum(recon_norm[i : i + 8] for i in range(0, subdim, 8))
        return 0

    lax.fori_loop(0, groups, one_group, 0)


def build(codes, codebook, residual, fold):
    subspaces, subdim, centroids = codebook.shape
    rows, width = residual.shape[0] // fold, residual.shape[1]
    groups = subspaces * subdim // LANES
    assert LANES % subdim == 0 and subdim % 8 == 0 and centroids % LANES == 0 and rows % LANES == 0
    return pl.pallas_call(
        build_kernel,
        in_specs=[pl.BlockSpec(memory_space=pltpu.HBM)] * 3,
        out_specs=[pl.BlockSpec(memory_space=pltpu.VMEM)] * 2,
        out_shape=[
            jax.ShapeDtypeStruct((2, width, rows), jnp.bfloat16),
            jax.ShapeDtypeStruct((16, rows), jnp.float32),
        ],
        scratch_shapes=[
            pltpu.VMEM((groups, LANES // subdim, rows), codes.dtype),
            pltpu.VMEM(codebook.shape, codebook.dtype),
            pltpu.VMEM((rows, width), residual.dtype),
            pltpu.SemaphoreType.DMA((3, groups)),
        ],
        compiler_params=pltpu.CompilerParams(vmem_limit_bytes=16 * 2**20),
        cost_estimate=pl.CostEstimate(
            flops=32 * rows * width, bytes_accessed=8 * rows * width, transcendentals=0
        ),
        name="build",
    )(in_hbm(codes), in_hbm(codebook), in_hbm(residual))


def count_kernel(order, visiting_ref, values_ref, norms_ref, out_ref, gathered):
    senders, count, packed = visiting_ref.shape
    width = values_ref.shape[1]
    for s in range(senders):
        gathered[s * count : (s + 1) * count, :] = visiting_ref[s].astype(jnp.float32)
    queries = gathered[:, :width]
    query_norms = jnp.sum(queries * queries, axis=1, keepdims=True)
    bounds = 1.9 + 0.6 * gathered[:, width : width + 1] / (LEVELS - 1)
    queries = queries.astype(jnp.bfloat16)

    def hit(kind):
        norms = jnp.sum(norms_ref[kind * 8 : kind * 8 + 8], axis=0, keepdims=True)
        cross = jnp.dot(queries, values_ref[kind], preferred_element_type=jnp.float32)
        distance = (query_norms + norms - 2.0 * cross) / width
        return jax.nn.sigmoid((bounds - distance) / 0.02)

    exact = hit(0)
    coarse = hit(1)
    lane = lax.broadcasted_iota(jnp.int32, (senders * count, LANES), 1)
    query = lax.broadcasted_iota(jnp.int32, (senders * count, LANES), 0)
    blocks = jnp.zeros((senders * count, LANES), jnp.float32)
    sums = jnp.zeros((1, LANES), jnp.float32)
    for k, values in enumerate((exact, coarse, exact * coarse)):
        total = jnp.sum(values, axis=1, keepdims=True)
        blocks = jnp.where(lane == k * count + query % count, total, blocks)
        sums = jnp.where(lane[:1] == 3 * count + k, jnp.sum(total, axis=0, keepdims=True), sums)
    for s in range(senders):
        row = jnp.sum(blocks[s * count : (s + 1) * count], axis=0, keepdims=True) + sums
        for p in range(out_ref.shape[0]):
            out_ref[p, order[s]] = row


def finish_kernel(fold, database, everyone, arrived_ref, hits_ref, totals_ref):
    copies, shards = arrived_ref.shape[:2]
    count = hits_ref.shape[1]
    mine = lax.axis_index("pb") // fold
    hits = jnp.zeros((1, LANES), jnp.float32)
    totals = jnp.zeros((1, LANES), jnp.float32)
    for p in range(copies):
        arrived = jnp.sum(arrived_ref[p], axis=0)
        hits += jnp.where(mine == p // fold, arrived, 0.0)
        totals += arrived
    hits = hits / database
    totals = totals / (database * everyone)
    for k in range(3):
        hits_ref[k : k + 1, :] = hits[:, k * count : (k + 1) * count]
    totals_ref[...] = totals[:, 3 * count : 3 * count + 3]


def per_device(queries, residual, codes, codebook, ranks):
    count, width = queries.shape
    shards, copies = lax.axis_size("db"), lax.axis_size("pb")
    devices = shards * copies
    fold = 2 if copies % 2 == 0 and residual.shape[0] % (2 * LANES) == 0 else 1
    rows = residual.shape[0] // fold
    senders = fold * shards
    assert 3 * count + 3 <= LANES

    order = list(range(senders))
    order.insert(0, order.pop(senders - shards // 2))
    groups = [[first + at for at in order] for first in range(0, devices, senders)]
    visiting = lax.all_to_all(
        pack(queries, ranks, senders), ("pb", "db"), 0, 0, axis_index_groups=groups
    )
    values, norms = build(codes.T, jnp.transpose(codebook, (0, 2, 1)), residual, fold)
    partial_sums = pl.pallas_call(
        functools.partial(count_kernel, order),
        out_shape=jax.ShapeDtypeStruct((copies // fold, senders, 1, LANES), jnp.float32),
        scratch_shapes=[pltpu.VMEM((senders * count, width + LANES), jnp.float32)],
        compiler_params=pltpu.CompilerParams(vmem_limit_bytes=16 * 2**20),
        cost_estimate=pl.CostEstimate(
            flops=4 * senders * count * rows * width,
            bytes_accessed=4 * rows * width,
            transcendentals=0,
        ),
        name="count",
    )(visiting, values, norms)
    arrived = lax.all_to_all(partial_sums.reshape(devices, 1, LANES), ("pb", "db"), 0, 0)
    hits, totals = pl.pallas_call(
        functools.partial(finish_kernel, fold, rows * senders, count * devices),
        out_shape=[
            jax.ShapeDtypeStruct((3, count), jnp.float32),
            jax.ShapeDtypeStruct((1, 3), jnp.float32),
        ],
        compiler_params=pltpu.CompilerParams(vmem_limit_bytes=8 * 2**20),
        name="finish",
    )(arrived.reshape(copies, shards, 1, LANES))
    return hits, totals[0]


def solution(mesh):
    return jax.shard_map(
        per_device,
        mesh=mesh,
        in_specs=(P(("pb", "db"), None), P("db", None), P("db", None), P(), P(("pb", "db"))),
        out_specs=(P(None, ("pb", "db")), P()),
        check_vma=False,
    )
```

```python
import functools
import math

import jax
import jax.numpy as jnp
from jax import lax
from jax.experimental import pallas as pl
from jax.experimental.pallas import tpu as pltpu
from jax.sharding import PartitionSpec as P

LEVELS = 64
LANES = 128


def in_hbm(array):
    return pltpu.with_memory_space_constraint(array, pltpu.HBM)


def pack_kernel(queries_hbm, ranks_hbm, out_ref, queries, ranks, sems):
    count, width = queries.shape
    copies = (
        pltpu.make_async_copy(ranks_hbm, ranks, sems.at[1]),
        pltpu.make_async_copy(queries_hbm, queries, sems.at[0]),
    )
    for copy in copies:
        copy.start()
    for copy in copies:
        copy.wait()
    for i in range(count):
        rank = jnp.full((1, LANES), ranks[i], jnp.int32).astype(jnp.float32)
        for s in range(out_ref.shape[0]):
            out_ref[s, i : i + 1, width:] = rank.astype(jnp.bfloat16)
    for s in range(out_ref.shape[0]):
        out_ref[s, :, :width] = queries[...]


def pack(queries, ranks, receivers):
    count, width = queries.shape
    return pl.pallas_call(
        pack_kernel,
        in_specs=[pl.BlockSpec(memory_space=pltpu.HBM)] * 2,
        out_shape=jax.ShapeDtypeStruct((receivers, count, width + LANES), jnp.bfloat16),
        scratch_shapes=[
            pltpu.VMEM(queries.shape, queries.dtype),
            pltpu.SMEM(ranks.shape, ranks.dtype),
            pltpu.SemaphoreType.DMA((2,)),
        ],
        compiler_params=pltpu.CompilerParams(vmem_limit_bytes=8 * 2**20),
        name="pack",
    )(in_hbm(queries), in_hbm(ranks))


def build_kernel(
    codes_hbm, codebook_hbm, residual_hbm, values_ref, norms_ref, codes, codebook, residual, sems
):
    subspaces, subdim, centroids = codebook.shape
    rows, width = residual.shape
    group = LANES // subdim
    groups = subspaces // group
    share = lax.rem(lax.axis_index("pb"), codes_hbm.shape[1] // rows)
    own = pl.ds(pl.multiple_of(share * rows, rows), rows)

    def copies(g):
        members = pl.ds(pl.multiple_of(g * group, group), group)
        features = pl.ds(pl.multiple_of(g * LANES, LANES), LANES)
        return (
            pltpu.make_async_copy(codes_hbm.at[members, own], codes.at[g], sems.at[0, g]),
            pltpu.make_async_copy(codebook_hbm.at[members], codebook.at[members], sems.at[1, g]),
            pltpu.make_async_copy(
                residual_hbm.at[own, features], residual.at[:, features], sems.at[2, g]
            ),
        )

    for g in range(groups):
        for copy in copies(g):
            copy.start()
    norms_ref[...] = jnp.zeros_like(norms_ref)
    row = lax.broadcasted_iota(jnp.int32, (LANES, LANES), 0)
    column = lax.broadcasted_iota(jnp.int32, (LANES, LANES), 1)
    identity = (row == column).astype(jnp.bfloat16)

    def one_group(g, _):
        for copy in copies(g):
            copy.wait()
        first = pl.multiple_of(g * LANES, LANES)
        for tile in range(rows // LANES):
            at = slice(tile * LANES, (tile + 1) * LANES)
            turned = lax.dot_general(
                identity,
                residual[at, pl.ds(first, LANES)],
                (((1,), (1,)), ((), ())),
                preferred_element_type=jnp.float32,
            )
            recon_norm = jnp.zeros((subdim, LANES), jnp.float32)
            vector_norm = jnp.zeros((subdim, LANES), jnp.float32)
            for m in range(group):
                code = jnp.broadcast_to(codes[g, m : m + 1, at], (subdim, LANES))
                lane = code & (LANES - 1)
                recon = None
                for part in range(centroids // LANES):
                    table = codebook[g * group + m, :, part * LANES : (part + 1) * LANES]
                    picked = jnp.take_along_axis(table, lane, axis=1, mode="promise_in_bounds")
                    recon = picked if part == 0 else jnp.where(code >= part * LANES, picked, recon)
                vector = (recon + turned[m * subdim : (m + 1) * subdim]).astype(jnp.bfloat16)
                rounded = recon.astype(jnp.bfloat16)
                recon_norm += rounded.astype(jnp.float32) ** 2
                vector_norm += vector.astype(jnp.float32) ** 2
                features = pl.ds(first + m * subdim, subdim)
                values_ref[0, features, at] = vector
                values_ref[1, features, at] = rounded
            norms_ref[0:8, at] += sum(vector_norm[i : i + 8] for i in range(0, subdim, 8))
            norms_ref[8:16, at] += sum(recon_norm[i : i + 8] for i in range(0, subdim, 8))
        return 0

    lax.fori_loop(0, groups, one_group, 0)


def build(codes, codebook, residual, fold):
    subspaces, subdim, centroids = codebook.shape
    rows, width = residual.shape[0] // fold, residual.shape[1]
    groups = subspaces * subdim // LANES
    assert LANES % subdim == 0 and subdim % 8 == 0 and centroids % LANES == 0 and rows % LANES == 0
    return pl.pallas_call(
        build_kernel,
        in_specs=[pl.BlockSpec(memory_space=pltpu.HBM)] * 3,
        out_specs=[pl.BlockSpec(memory_space=pltpu.VMEM)] * 2,
        out_shape=[
            jax.ShapeDtypeStruct((2, width, rows), jnp.bfloat16),
            jax.ShapeDtypeStruct((16, rows), jnp.float32),
        ],
        scratch_shapes=[
            pltpu.VMEM((groups, LANES // subdim, rows), codes.dtype),
            pltpu.VMEM(codebook.shape, codebook.dtype),
            pltpu.VMEM((rows, width), residual.dtype),
            pltpu.SemaphoreType.DMA((3, groups)),
        ],
        compiler_params=pltpu.CompilerParams(vmem_limit_bytes=16 * 2**20),
        cost_estimate=pl.CostEstimate(
            flops=32 * rows * width, bytes_accessed=8 * rows * width, transcendentals=0
        ),
        name="build",
    )(in_hbm(codes), in_hbm(codebook), in_hbm(residual))


def count_kernel(order, visiting_ref, values_ref, norms_ref, out_ref, gathered):
    senders, count, packed = visiting_ref.shape
    width = values_ref.shape[1]
    for s in range(senders):
        gathered[s * count : (s + 1) * count, :] = visiting_ref[s].astype(jnp.float32)
    queries = gathered[:, :width]
    query_norms = jnp.sum(queries * queries, axis=1, keepdims=True)
    bounds = 1.9 + 0.6 * gathered[:, width : width + 1] / (LEVELS - 1)
    queries = queries.astype(jnp.bfloat16)

    def hit(kind):
        norms = jnp.sum(norms_ref[kind * 8 : kind * 8 + 8], axis=0, keepdims=True)
        cross = jnp.dot(queries, values_ref[kind], preferred_element_type=jnp.float32)
        distance = (query_norms + norms - 2.0 * cross) / width
        return jax.nn.sigmoid((bounds - distance) / 0.02)

    exact = hit(0)
    coarse = hit(1)
    lane = lax.broadcasted_iota(jnp.int32, (senders * count, LANES), 1)
    query = lax.broadcasted_iota(jnp.int32, (senders * count, LANES), 0)
    blocks = jnp.zeros((senders * count, LANES), jnp.float32)
    sums = jnp.zeros((1, LANES), jnp.float32)
    for k, values in enumerate((exact, coarse, exact * coarse)):
        total = jnp.sum(values, axis=1, keepdims=True)
        blocks = jnp.where(lane == k * count + query % count, total, blocks)
        sums = jnp.where(lane[:1] == 3 * count + k, jnp.sum(total, axis=0, keepdims=True), sums)
    for s in range(senders):
        row = jnp.sum(blocks[s * count : (s + 1) * count], axis=0, keepdims=True) + sums
        for p in range(out_ref.shape[0]):
            out_ref[p, order[s]] = row


def finish_kernel(fold, database, everyone, arrived_ref, hits_ref, totals_ref):
    copies, shards = arrived_ref.shape[:2]
    count = hits_ref.shape[1]
    mine = lax.axis_index("pb") // fold
    hits = jnp.zeros((1, LANES), jnp.float32)
    totals = jnp.zeros((1, LANES), jnp.float32)
    for p in range(copies):
        arrived = jnp.sum(arrived_ref[p], axis=0)
        hits += jnp.where(mine == p // fold, arrived, 0.0)
        totals += arrived
    hits = hits / database
    totals = totals / (database * everyone)
    for k in range(3):
        hits_ref[k : k + 1, :] = hits[:, k * count : (k + 1) * count]
    totals_ref[...] = totals[:, 3 * count : 3 * count + 3]


def per_device(queries, residual, codes, codebook, ranks):
    count, width = queries.shape
    shards, copies = lax.axis_size("db"), lax.axis_size("pb")
    devices = shards * copies
    fold = 2 if copies % 2 == 0 and residual.shape[0] % (2 * LANES) == 0 else 1
    rows = residual.shape[0] // fold
    senders = fold * shards
    assert 3 * count + 3 <= LANES

    stride = senders // 2 - 1 if math.gcd(senders // 2 - 1, senders) == 1 else 1
    order = [(senders - shards // 2 - 1 + stride * i) % senders for i in range(senders)]
    groups = [[first + at for at in order] for first in range(0, devices, senders)]
    visiting = lax.all_to_all(
        pack(queries, ranks, senders), ("pb", "db"), 0, 0, axis_index_groups=groups
    )
    values, norms = build(codes.T, jnp.transpose(codebook, (0, 2, 1)), residual, fold)
    partial_sums = pl.pallas_call(
        functools.partial(count_kernel, order),
        out_shape=jax.ShapeDtypeStruct((copies // fold, senders, 1, LANES), jnp.float32),
        scratch_shapes=[pltpu.VMEM((senders * count, width + LANES), jnp.float32)],
        compiler_params=pltpu.CompilerParams(vmem_limit_bytes=16 * 2**20),
        cost_estimate=pl.CostEstimate(
            flops=4 * senders * count * rows * width,
            bytes_accessed=4 * rows * width,
            transcendentals=0,
        ),
        name="count",
    )(visiting, values, norms)
    arrived = lax.all_to_all(partial_sums.reshape(devices, 1, LANES), ("pb", "db"), 0, 0)
    hits, totals = pl.pallas_call(
        functools.partial(finish_kernel, fold, rows * senders, count * devices),
        out_shape=[
            jax.ShapeDtypeStruct((3, count), jnp.float32),
            jax.ShapeDtypeStruct((1, 3), jnp.float32),
        ],
        compiler_params=pltpu.CompilerParams(vmem_limit_bytes=8 * 2**20),
        name="finish",
    )(arrived.reshape(copies, shards, 1, LANES))
    return hits, totals[0]


def solution(mesh):
    return jax.shard_map(
        per_device,
        mesh=mesh,
        in_specs=(P(("pb", "db"), None), P("db", None), P("db", None), P(), P(("pb", "db"))),
        out_specs=(P(None, ("pb", "db")), P()),
        check_vma=False,
    )
```

```python
import functools
import math

import jax
import jax.numpy as jnp
from jax import lax
from jax.experimental import pallas as pl
from jax.experimental.pallas import tpu as pltpu
from jax.sharding import PartitionSpec as P

LEVELS = 64
LANES = 128


def in_hbm(array):
    return pltpu.with_memory_space_constraint(array, pltpu.HBM)


def pack_kernel(queries_hbm, ranks_hbm, out_ref, queries, ranks, sems):
    count, width = queries.shape
    copies = (
        pltpu.make_async_copy(ranks_hbm, ranks, sems.at[1]),
        pltpu.make_async_copy(queries_hbm, queries, sems.at[0]),
    )
    for copy in copies:
        copy.start()
    for copy in copies:
        copy.wait()
    receivers, lines, _ = out_ref.shape
    line = lax.broadcasted_iota(jnp.int32, (lines, LANES), 0)
    lane = lax.broadcasted_iota(jnp.int32, (lines, LANES), 1)
    rank = jnp.zeros((lines, LANES), jnp.int32)
    for i in range(count):
        rank = jnp.where((line == i % lines) & (lane == i // lines), ranks[i], rank)
    rank = rank.astype(jnp.float32).astype(jnp.bfloat16)
    parts = [queries[i * lines : (i + 1) * lines, :] for i in range(count // lines)]
    for s in range(receivers):
        for i, part in enumerate(parts):
            out_ref[s, :, i * width : (i + 1) * width] = part
        out_ref[s, :, len(parts) * width :] = rank


def pack(queries, ranks, receivers, lines):
    count, width = queries.shape
    return pl.pallas_call(
        pack_kernel,
        in_specs=[pl.BlockSpec(memory_space=pltpu.HBM)] * 2,
        out_shape=jax.ShapeDtypeStruct(
            (receivers, lines, count // lines * width + LANES), jnp.bfloat16
        ),
        scratch_shapes=[
            pltpu.VMEM(queries.shape, queries.dtype),
            pltpu.SMEM(ranks.shape, ranks.dtype),
            pltpu.SemaphoreType.DMA((2,)),
        ],
        compiler_params=pltpu.CompilerParams(vmem_limit_bytes=8 * 2**20),
        name="pack",
    )(in_hbm(queries), in_hbm(ranks))


def build_kernel(
    codes_hbm, codebook_hbm, residual_hbm, values_ref, norms_ref, codes, codebook, residual, sems
):
    subspaces, subdim, centroids = codebook.shape
    rows, width = residual.shape
    group = LANES // subdim
    groups = subspaces // group
    share = lax.rem(lax.axis_index("pb"), codes_hbm.shape[1] // rows)
    own = pl.ds(pl.multiple_of(share * rows, rows), rows)

    def copies(g):
        members = pl.ds(pl.multiple_of(g * group, group), group)
        features = pl.ds(pl.multiple_of(g * LANES, LANES), LANES)
        return (
            pltpu.make_async_copy(codes_hbm.at[members, own], codes.at[g], sems.at[0, g]),
            pltpu.make_async_copy(codebook_hbm.at[members], codebook.at[members], sems.at[1, g]),
            pltpu.make_async_copy(
                residual_hbm.at[own, features], residual.at[:, features], sems.at[2, g]
            ),
        )

    for g in range(groups):
        for copy in copies(g):
            copy.start()
    norms_ref[...] = jnp.zeros_like(norms_ref)
    row = lax.broadcasted_iota(jnp.int32, (LANES, LANES), 0)
    column = lax.broadcasted_iota(jnp.int32, (LANES, LANES), 1)
    identity = (row == column).astype(jnp.bfloat16)

    def one_group(g, _):
        for copy in copies(g):
            copy.wait()
        first = pl.multiple_of(g * LANES, LANES)
        for tile in range(rows // LANES):
            at = slice(tile * LANES, (tile + 1) * LANES)
            turned = lax.dot_general(
                identity,
                residual[at, pl.ds(first, LANES)],
                (((1,), (1,)), ((), ())),
                preferred_element_type=jnp.float32,
            )
            recon_norm = jnp.zeros((subdim, LANES), jnp.float32)
            vector_norm = jnp.zeros((subdim, LANES), jnp.float32)
            for m in range(group):
                code = jnp.broadcast_to(codes[g, m : m + 1, at], (subdim, LANES))
                lane = code & (LANES - 1)
                recon = None
                for part in range(centroids // LANES):
                    table = codebook[g * group + m, :, part * LANES : (part + 1) * LANES]
                    picked = jnp.take_along_axis(table, lane, axis=1, mode="promise_in_bounds")
                    recon = picked if part == 0 else jnp.where(code >= part * LANES, picked, recon)
                vector = (recon + turned[m * subdim : (m + 1) * subdim]).astype(jnp.bfloat16)
                rounded = recon.astype(jnp.bfloat16)
                recon_norm += rounded.astype(jnp.float32) ** 2
                vector_norm += vector.astype(jnp.float32) ** 2
                features = pl.ds(first + m * subdim, subdim)
                values_ref[0, features, at] = vector
                values_ref[1, features, at] = rounded
            norms_ref[0:8, at] += sum(vector_norm[i : i + 8] for i in range(0, subdim, 8))
            norms_ref[8:16, at] += sum(recon_norm[i : i + 8] for i in range(0, subdim, 8))
        return 0

    lax.fori_loop(0, groups, one_group, 0)


def build(codes, codebook, residual, fold):
    subspaces, subdim, centroids = codebook.shape
    rows, width = residual.shape[0] // fold, residual.shape[1]
    groups = subspaces * subdim // LANES
    assert LANES % subdim == 0 and subdim % 8 == 0 and centroids % LANES == 0 and rows % LANES == 0
    return pl.pallas_call(
        build_kernel,
        in_specs=[pl.BlockSpec(memory_space=pltpu.HBM)] * 3,
        out_specs=[pl.BlockSpec(memory_space=pltpu.VMEM)] * 2,
        out_shape=[
            jax.ShapeDtypeStruct((2, width, rows), jnp.bfloat16),
            jax.ShapeDtypeStruct((16, rows), jnp.float32),
        ],
        scratch_shapes=[
            pltpu.VMEM((groups, LANES // subdim, rows), codes.dtype),
            pltpu.VMEM(codebook.shape, codebook.dtype),
            pltpu.VMEM((rows, width), residual.dtype),
            pltpu.SemaphoreType.DMA((3, groups)),
        ],
        compiler_params=pltpu.CompilerParams(vmem_limit_bytes=16 * 2**20),
        cost_estimate=pl.CostEstimate(
            flops=32 * rows * width, bytes_accessed=8 * rows * width, transcendentals=0
        ),
        name="build",
    )(in_hbm(codes), in_hbm(codebook), in_hbm(residual))


def count_kernel(order, visiting_ref, values_ref, norms_ref, out_ref, gathered):
    senders, lines, _ = visiting_ref.shape
    width = values_ref.shape[1]
    parts = gathered.shape[0] // (senders * lines)
    count = parts * lines
    for s in range(senders):
        tail = visiting_ref[s, :, parts * width :].astype(jnp.float32)
        for i in range(parts):
            rows = slice((i * senders + s) * lines, (i * senders + s + 1) * lines)
            part = visiting_ref[s, :, i * width : (i + 1) * width]
            gathered[rows, :width] = part.astype(jnp.float32)
            gathered[rows, width:] = jnp.broadcast_to(tail[:, i : i + 1], (lines, LANES))
    queries = gathered[:, :width]
    query_norms = jnp.sum(queries * queries, axis=1, keepdims=True)
    bounds = 1.9 + 0.6 * gathered[:, width : width + 1] / (LEVELS - 1)
    queries = queries.astype(jnp.bfloat16)

    def hit(kind):
        norms = jnp.sum(norms_ref[kind * 8 : kind * 8 + 8], axis=0, keepdims=True)
        cross = jnp.dot(queries, values_ref[kind], preferred_element_type=jnp.float32)
        distance = (query_norms + norms - 2.0 * cross) / width
        return jax.nn.sigmoid((bounds - distance) / 0.02)

    exact = hit(0)
    coarse = hit(1)
    lane = lax.broadcasted_iota(jnp.int32, (senders * count, LANES), 1)
    query = lax.broadcasted_iota(jnp.int32, (senders * count, LANES), 0)
    blocks = jnp.zeros((senders * count, LANES), jnp.float32)
    sums = jnp.zeros((1, LANES), jnp.float32)
    for k, values in enumerate((exact, coarse, exact * coarse)):
        total = jnp.sum(values, axis=1, keepdims=True)
        mine = query // (senders * lines) * lines + query % lines
        blocks = jnp.where(lane == k * count + mine, total, blocks)
        sums = jnp.where(lane[:1] == 3 * count + k, jnp.sum(total, axis=0, keepdims=True), sums)
    for s in range(senders):
        row = sums
        for i in range(parts):
            first = (i * senders + s) * lines
            row += jnp.sum(blocks[first : first + lines], axis=0, keepdims=True)
        for p in range(out_ref.shape[0]):
            out_ref[p, order[s]] = row


def finish_kernel(fold, database, everyone, arrived_ref, hits_ref, totals_ref):
    copies, shards = arrived_ref.shape[:2]
    count = hits_ref.shape[1]
    mine = lax.axis_index("pb") // fold
    hits = jnp.zeros((1, LANES), jnp.float32)
    totals = jnp.zeros((1, LANES), jnp.float32)
    for p in range(copies):
        arrived = jnp.sum(arrived_ref[p], axis=0)
        hits += jnp.where(mine == p // fold, arrived, 0.0)
        totals += arrived
    hits = hits / database
    totals = totals / (database * everyone)
    for k in range(3):
        hits_ref[k : k + 1, :] = hits[:, k * count : (k + 1) * count]
    totals_ref[...] = totals[:, 3 * count : 3 * count + 3]


def per_device(queries, residual, codes, codebook, ranks):
    count, width = queries.shape
    shards, copies = lax.axis_size("db"), lax.axis_size("pb")
    devices = shards * copies
    fold = 2 if copies % 2 == 0 and residual.shape[0] % (2 * LANES) == 0 else 1
    rows = residual.shape[0] // fold
    senders = fold * shards
    lines = 2 if count % 2 == 0 else count
    assert 3 * count + 3 <= LANES

    stride = senders // 2 - 1 if math.gcd(senders // 2 - 1, senders) == 1 else 1
    order = [(senders - shards // 2 - 1 + stride * i) % senders for i in range(senders)]
    groups = [[first + at for at in order] for first in range(0, devices, senders)]
    visiting = lax.all_to_all(
        pack(queries, ranks, senders, lines), ("pb", "db"), 0, 0, axis_index_groups=groups
    )
    values, norms = build(codes.T, jnp.transpose(codebook, (0, 2, 1)), residual, fold)
    partial_sums = pl.pallas_call(
        functools.partial(count_kernel, order),
        out_shape=jax.ShapeDtypeStruct((copies // fold, senders, 1, LANES), jnp.float32),
        scratch_shapes=[pltpu.VMEM((senders * count, width + LANES), jnp.float32)],
        compiler_params=pltpu.CompilerParams(vmem_limit_bytes=16 * 2**20),
        cost_estimate=pl.CostEstimate(
            flops=4 * senders * count * rows * width,
            bytes_accessed=4 * rows * width,
            transcendentals=0,
        ),
        name="count",
    )(visiting, values, norms)
    arrived = lax.all_to_all(partial_sums.reshape(devices, 1, LANES), ("pb", "db"), 0, 0)
    hits, totals = pl.pallas_call(
        functools.partial(finish_kernel, fold, rows * senders, count * devices),
        out_shape=[
            jax.ShapeDtypeStruct((3, count), jnp.float32),
            jax.ShapeDtypeStruct((1, 3), jnp.float32),
        ],
        compiler_params=pltpu.CompilerParams(vmem_limit_bytes=8 * 2**20),
        name="finish",
    )(arrived.reshape(copies, shards, 1, LANES))
    return hits, totals[0]


def solution(mesh):
    return jax.shard_map(
        per_device,
        mesh=mesh,
        in_specs=(P(("pb", "db"), None), P("db", None), P("db", None), P(), P(("pb", "db"))),
        out_specs=(P(None, ("pb", "db")), P()),
        check_vma=False,
    )
```

```python
import functools
import math

import jax
import jax.numpy as jnp
from jax import lax
from jax.experimental import pallas as pl
from jax.experimental.pallas import tpu as pltpu
from jax.sharding import PartitionSpec as P

LEVELS = 64
LANES = 128


def in_hbm(array):
    return pltpu.with_memory_space_constraint(array, pltpu.HBM)


def pack_kernel(queries_hbm, ranks_hbm, out_ref, queries, ranks, sems):
    count, width = queries.shape
    copies = (
        pltpu.make_async_copy(ranks_hbm, ranks, sems.at[1]),
        pltpu.make_async_copy(queries_hbm, queries, sems.at[0]),
    )
    for copy in copies:
        copy.start()
    for copy in copies:
        copy.wait()
    receivers, lines, _ = out_ref.shape
    line = lax.broadcasted_iota(jnp.int32, (lines, LANES), 0)
    lane = lax.broadcasted_iota(jnp.int32, (lines, LANES), 1)
    rank = jnp.zeros((lines, LANES), jnp.int32)
    for i in range(count):
        rank = jnp.where((line == i % lines) & (lane == i // lines), ranks[i], rank)
    rank = rank.astype(jnp.float32).astype(jnp.bfloat16)
    parts = [queries[i * lines : (i + 1) * lines, :] for i in range(count // lines)]
    for s in range(receivers):
        for i, part in enumerate(parts):
            out_ref[s, :, i * width : (i + 1) * width] = part
        out_ref[s, :, len(parts) * width :] = rank


def pack(queries, ranks, receivers, lines):
    count, width = queries.shape
    return pl.pallas_call(
        pack_kernel,
        in_specs=[pl.BlockSpec(memory_space=pltpu.HBM)] * 2,
        out_shape=jax.ShapeDtypeStruct(
            (receivers, lines, count // lines * width + LANES), jnp.bfloat16
        ),
        scratch_shapes=[
            pltpu.VMEM(queries.shape, queries.dtype),
            pltpu.SMEM(ranks.shape, ranks.dtype),
            pltpu.SemaphoreType.DMA((2,)),
        ],
        compiler_params=pltpu.CompilerParams(vmem_limit_bytes=8 * 2**20),
        name="pack",
    )(in_hbm(queries), in_hbm(ranks))


def build_kernel(
    codes_hbm, codebook_hbm, residual_hbm, values_ref, norms_ref, codes, codebook, residual, sems
):
    subspaces, subdim, centroids = codebook.shape
    rows, width = residual.shape
    group = LANES // subdim
    groups = subspaces // group
    share = lax.rem(lax.axis_index("pb"), codes_hbm.shape[1] // rows)
    own = pl.ds(pl.multiple_of(share * rows, rows), rows)

    def copies(g):
        members = pl.ds(pl.multiple_of(g * group, group), group)
        features = pl.ds(pl.multiple_of(g * LANES, LANES), LANES)
        return (
            pltpu.make_async_copy(codes_hbm.at[members, own], codes.at[g], sems.at[0, g]),
            pltpu.make_async_copy(codebook_hbm.at[members], codebook.at[members], sems.at[1, g]),
            pltpu.make_async_copy(
                residual_hbm.at[own, features], residual.at[:, features], sems.at[2, g]
            ),
        )

    for g in range(groups):
        for copy in copies(g):
            copy.start()
    norms_ref[...] = jnp.zeros_like(norms_ref)
    row = lax.broadcasted_iota(jnp.int32, (LANES, LANES), 0)
    column = lax.broadcasted_iota(jnp.int32, (LANES, LANES), 1)
    identity = (row == column).astype(jnp.bfloat16)

    def one_group(g, _):
        for copy in copies(g):
            copy.wait()
        first = pl.multiple_of(g * LANES, LANES)
        for tile in range(rows // LANES):
            at = slice(tile * LANES, (tile + 1) * LANES)
            turned = lax.dot_general(
                identity,
                residual[at, pl.ds(first, LANES)],
                (((1,), (1,)), ((), ())),
                preferred_element_type=jnp.float32,
            )
            recon_norm = jnp.zeros((subdim, LANES), jnp.float32)
            vector_norm = jnp.zeros((subdim, LANES), jnp.float32)
            for m in range(group):
                code = jnp.broadcast_to(codes[g, m : m + 1, at], (subdim, LANES))
                lane = code & (LANES - 1)
                recon = None
                for part in range(centroids // LANES):
                    table = codebook[g * group + m, :, part * LANES : (part + 1) * LANES]
                    picked = jnp.take_along_axis(table, lane, axis=1, mode="promise_in_bounds")
                    recon = picked if part == 0 else jnp.where(code >= part * LANES, picked, recon)
                vector = (recon + turned[m * subdim : (m + 1) * subdim]).astype(jnp.bfloat16)
                rounded = recon.astype(jnp.bfloat16)
                recon_norm += rounded.astype(jnp.float32) ** 2
                vector_norm += vector.astype(jnp.float32) ** 2
                features = pl.ds(first + m * subdim, subdim)
                values_ref[0, features, at] = vector
                values_ref[1, features, at] = rounded
            norms_ref[0:8, at] += sum(vector_norm[i : i + 8] for i in range(0, subdim, 8))
            norms_ref[8:16, at] += sum(recon_norm[i : i + 8] for i in range(0, subdim, 8))
        return 0

    lax.fori_loop(0, groups, one_group, 0)


def build(codes, codebook, residual, fold):
    subspaces, subdim, centroids = codebook.shape
    rows, width = residual.shape[0] // fold, residual.shape[1]
    groups = subspaces * subdim // LANES
    assert LANES % subdim == 0 and subdim % 8 == 0 and centroids % LANES == 0 and rows % LANES == 0
    return pl.pallas_call(
        build_kernel,
        in_specs=[pl.BlockSpec(memory_space=pltpu.HBM)] * 3,
        out_specs=[pl.BlockSpec(memory_space=pltpu.VMEM)] * 2,
        out_shape=[
            jax.ShapeDtypeStruct((2, width, rows), jnp.bfloat16),
            jax.ShapeDtypeStruct((16, rows), jnp.float32),
        ],
        scratch_shapes=[
            pltpu.VMEM((groups, LANES // subdim, rows), codes.dtype),
            pltpu.VMEM(codebook.shape, codebook.dtype),
            pltpu.VMEM((rows, width), residual.dtype),
            pltpu.SemaphoreType.DMA((3, groups)),
        ],
        compiler_params=pltpu.CompilerParams(vmem_limit_bytes=16 * 2**20),
        cost_estimate=pl.CostEstimate(
            flops=32 * rows * width, bytes_accessed=8 * rows * width, transcendentals=0
        ),
        name="build",
    )(in_hbm(codes), in_hbm(codebook), in_hbm(residual))


def count_kernel(order, visiting_ref, values_ref, norms_ref, out_ref, gathered):
    senders, lines, _ = visiting_ref.shape
    width = values_ref.shape[1]
    parts = gathered.shape[0] // (senders * lines)
    count = parts * lines
    for s in range(senders):
        tail = visiting_ref[s, :, parts * width :].astype(jnp.float32)
        for i in range(parts):
            rows = slice((i * senders + s) * lines, (i * senders + s + 1) * lines)
            part = visiting_ref[s, :, i * width : (i + 1) * width]
            gathered[rows, :width] = part.astype(jnp.float32)
            gathered[rows, width:] = jnp.broadcast_to(tail[:, i : i + 1], (lines, LANES))
    queries = gathered[:, :width]
    query_norms = jnp.sum(queries * queries, axis=1, keepdims=True)
    bounds = 1.9 + 0.6 * gathered[:, width : width + 1] / (LEVELS - 1)
    queries = queries.astype(jnp.bfloat16)

    def hit(kind):
        norms = jnp.sum(norms_ref[kind * 8 : kind * 8 + 8], axis=0, keepdims=True)
        cross = jnp.dot(queries, values_ref[kind], preferred_element_type=jnp.float32)
        distance = (query_norms + norms - 2.0 * cross) / width
        return jax.nn.sigmoid((bounds - distance) / 0.02)

    exact = hit(0)
    coarse = hit(1)
    lane = lax.broadcasted_iota(jnp.int32, (senders * count, LANES), 1)
    query = lax.broadcasted_iota(jnp.int32, (senders * count, LANES), 0)
    blocks = jnp.zeros((senders * count, LANES), jnp.float32)
    sums = jnp.zeros((1, LANES), jnp.float32)
    for k, values in enumerate((exact, coarse, exact * coarse)):
        total = jnp.sum(values, axis=1, keepdims=True)
        mine = query // (senders * lines) * lines + query % lines
        blocks = jnp.where(lane == k * count + mine, total, blocks)
        sums = jnp.where(lane[:1] == 3 * count + k, jnp.sum(total, axis=0, keepdims=True), sums)
    for s in range(senders):
        row = sums
        for i in range(parts):
            first = (i * senders + s) * lines
            row += jnp.sum(blocks[first : first + lines], axis=0, keepdims=True)
        for p in range(out_ref.shape[0]):
            out_ref[p, order[s]] = row


def finish_kernel(fold, database, everyone, arrived_ref, hits_ref, totals_ref):
    copies, shards = arrived_ref.shape[:2]
    count = hits_ref.shape[1]
    mine = lax.axis_index("pb") // fold
    hits = jnp.zeros((1, LANES), jnp.float32)
    totals = jnp.zeros((1, LANES), jnp.float32)
    for p in range(copies):
        arrived = jnp.sum(arrived_ref[p], axis=0)
        hits += jnp.where(mine == p // fold, arrived, 0.0)
        totals += arrived
    hits = hits / database
    totals = totals / (database * everyone)
    for k in range(3):
        hits_ref[k : k + 1, :] = hits[:, k * count : (k + 1) * count]
    totals_ref[...] = totals[:, 3 * count : 3 * count + 3]


def per_device(queries, residual, codes, codebook, ranks):
    count, width = queries.shape
    shards, copies = lax.axis_size("db"), lax.axis_size("pb")
    devices = shards * copies
    fold = 2 if copies % 2 == 0 and residual.shape[0] % (2 * LANES) == 0 else 1
    rows = residual.shape[0] // fold
    senders = fold * shards
    lines = 2 if count % 2 == 0 else count
    assert 3 * count + 3 <= LANES

    stride = senders // 2 - 1 if math.gcd(senders // 2 - 1, senders) == 1 else 1
    order = [(senders - shards // 2 + stride * i) % senders for i in range(senders)]
    groups = [[first + at for at in order] for first in range(0, devices, senders)]
    visiting = lax.all_to_all(
        pack(queries, ranks, senders, lines), ("pb", "db"), 0, 0, axis_index_groups=groups
    )
    values, norms = build(codes.T, jnp.transpose(codebook, (0, 2, 1)), residual, fold)
    partial_sums = pl.pallas_call(
        functools.partial(count_kernel, order),
        out_shape=jax.ShapeDtypeStruct((copies // fold, senders, 1, LANES), jnp.float32),
        scratch_shapes=[pltpu.VMEM((senders * count, width + LANES), jnp.float32)],
        compiler_params=pltpu.CompilerParams(vmem_limit_bytes=16 * 2**20),
        cost_estimate=pl.CostEstimate(
            flops=4 * senders * count * rows * width,
            bytes_accessed=4 * rows * width,
            transcendentals=0,
        ),
        name="count",
    )(visiting, values, norms)
    arrived = lax.all_to_all(partial_sums.reshape(devices, 1, LANES), ("pb", "db"), 0, 0)
    hits, totals = pl.pallas_call(
        functools.partial(finish_kernel, fold, rows * senders, count * devices),
        out_shape=[
            jax.ShapeDtypeStruct((3, count), jnp.float32),
            jax.ShapeDtypeStruct((1, 3), jnp.float32),
        ],
        compiler_params=pltpu.CompilerParams(vmem_limit_bytes=8 * 2**20),
        name="finish",
    )(arrived.reshape(copies, shards, 1, LANES))
    return hits, totals[0]


def solution(mesh):
    return jax.shard_map(
        per_device,
        mesh=mesh,
        in_specs=(P(("pb", "db"), None), P("db", None), P("db", None), P(), P(("pb", "db"))),
        out_specs=(P(None, ("pb", "db")), P()),
        check_vma=False,
    )
```
